256 devices in a mesh: fsdp: 32 (over y, x, z_lo), rep: 8 (over z_hi, core).
Axes of the slice: x: 4, y: 4, z: 8 (z_hi: 4, z_lo: 2; z = z_hi * 2 + z_lo), core: 2. Of those that a mesh axis runs over, the one named last changes fastest.
Arguments:
- tokens: bfloat16 [122880, 3584], P(('fsdp', 'rep')), may hold values from -6 to 6
- positions: int32 [122880], P(('fsdp', 'rep')), may hold values from 0 to 4095
- slow_weight: float32 [3584, 4096], P('fsdp', 'rep'), may hold values from -0.09375 to 0.09375
- fast_weight: bfloat16 [8, 3584, 4096], P('rep', 'fsdp'), may hold values from -0.125 to 0.125
- slow_gain: float32 [3584], P(('fsdp', 'rep')), may hold values from -3 to 3
- fast_gain: bfloat16 [8, 3584], P('rep', 'fsdp'), may hold values from -3 to 3
Outputs:
- query_states: bfloat16 [122880, 2048], P(('fsdp', 'rep'))
- key_states: bfloat16 [122880, 1024], P(('fsdp', 'rep'))
- value_states: bfloat16 [122880, 1024], P(('fsdp', 'rep'))
- new_weight: float32 [3584, 4096], P('fsdp', 'rep')
- new_gain: float32 [3584], P(('fsdp', 'rep'))
The draws below stay inside these ranges and needn't reach their ends.
All inputs are finite; a program needn't handle non-finite values.
Results may differ from the reference program's by a relative error of at most 0.012.
Values may be sent and summed in bfloat16 or wider, within the bound.
A program may use at most 128 MiB of HBM per device.

```python
import jax
import jax.numpy as jnp
from jax import lax

D = 3584
QHEADS = 8
KVHEADS = 4
HEAD = 256
QKV = 4096
TOKENS = 122880
N_REP = 8


def touch_ends(entries, stream_key, low, top_value):
    extent = entries.shape
    index_at = [jax.random.randint(jax.random.fold_in(stream_key, axis), (), 0, extent[axis]) for axis in range(len(extent))]
    entries = entries.at[tuple(index_at)].set(low)
    longest = extent.index(max(extent))
    index_at[longest] = (index_at[longest] + 1) % extent[longest]
    return entries.at[tuple(index_at)].set(top_value)


def raised(drawn, rng, source, target, blocks, factor):
    def block_of(axis_at):
        return (jnp.arange(drawn.shape[axis_at]) // (drawn.shape[axis_at] // blocks)).reshape((-1,) + (1,) * (drawn.ndim - 1 - axis_at))

    one_side = jax.random.permutation(rng, blocks)[block_of(target)]
    second = (block_of(target) + blocks // 2) % blocks
    return jnp.where((block_of(source) == one_side) | (block_of(source) == second), factor * drawn, drawn)


def block_scale(own_key, shape, shards, least, high):
    factor_of = 1.0
    for dim, shards_of in shards:
        heights = jax.random.uniform(jax.random.fold_in(jax.random.fold_in(own_key, 6), dim), (shards_of,), jnp.float32, least / len(shards), high / len(shards))
        factor_of = factor_of * jnp.repeat(jnp.exp(heights), shape[dim] // shards_of).reshape((-1,) + (1,) * (len(shape) - 1 - dim))
    return factor_of


def centred(rng, dims, width, reach, pieces=(), kind=jnp.bfloat16):
    gain = block_scale(rng, dims, pieces, -0.22, 0.18) if pieces else 1.0
    entries = jax.random.normal(rng, dims, jnp.float32) * width * gain
    return jnp.minimum(jnp.maximum(entries, -reach), reach).astype(kind)


def gaussian_with(key, shape, deviation, bound, pieces, heavy, held_as=jnp.bfloat16):
    result = deviation * jax.random.normal(key, shape, jnp.float32)
    if pieces:
        result = result * block_scale(key, shape, pieces, -0.22, 0.18)
    return jnp.clip(raised(result, jax.random.fold_in(key, 3), *heavy), -bound, bound).astype(held_as)


def setup_inputs(seed: int = 0) -> dict:
    keys = jax.random.split(jax.random.key(seed), 7)
    return {
        "tokens": centred(keys[0], (TOKENS, D), 1.0, 6.0, ((0, 256),)),
        "positions": touch_ends(jax.random.randint(keys[1], (TOKENS,), 0, 4096), jax.random.fold_in(keys[1], 1), 0, 4095).astype(jnp.int32),
        "slow_weight": centred(keys[2], (D, QKV), D ** -0.5, 0.09375, ((0, 32), (1, 8)), jnp.float32),
        "fast_weight": gaussian_with(keys[3], (N_REP, D, QKV), D ** -0.5, 0.125, ((0, 8), (1, 32)), (0, 2, 8, 2.0)),
        "slow_gain": centred(keys[4], (D,), 0.5, 3.0, ((0, 256),), jnp.float32),
        "fast_gain": gaussian_with(keys[5], (N_REP, D), 0.5, 3.0, ((0, 8), (1, 32)), (0, 1, 8, 2.0)),
    }


EPSILON = 1e-06
ADVANCE_RATE = 0.5
ROPE_BASE = 10000.0

def rotate(values, positions, head_count):
    row_count = values.shape[0]
    head_width = values.shape[1] // head_count
    half_width = head_width // 2
    by_head = values.reshape(row_count, head_count, head_width)
    inverse_rates = ROPE_BASE ** (-(jnp.arange(half_width, dtype=jnp.float32) * 2.0 / head_width))
    angles = positions.astype(jnp.float32)[:, None] * inverse_rates[None, :]
    cosine_table = jnp.cos(angles)[:, None, :]
    sine_table = jnp.sin(angles)[:, None, :]
    front_half = by_head[:, :, :half_width]
    back_half = by_head[:, :, half_width:]
    turned = jnp.concatenate([front_half * cosine_table - back_half * sine_table, back_half * cosine_table + front_half * sine_table], axis=2)
    return turned.reshape(row_count, head_count * head_width)

def reference(tokens, positions, slow_weight, fast_weight, slow_gain, fast_gain):
    mean_weight = lax.optimization_barrier(jnp.sum(fast_weight.astype(jnp.float32), axis=0)) / N_REP
    mean_gain = lax.optimization_barrier(jnp.sum(fast_gain.astype(jnp.float32), axis=0)) / N_REP
    new_weight = slow_weight + ADVANCE_RATE * (mean_weight - slow_weight)
    new_gain = slow_gain + ADVANCE_RATE * (mean_gain - slow_gain)
    layer_weight = new_weight.astype(jnp.bfloat16)
    layer_gain = new_gain.astype(jnp.bfloat16)
    floats = tokens.astype(jnp.float32)
    inv_rms = lax.rsqrt(lax.optimization_barrier(jnp.mean(floats * floats, axis=1, keepdims=True)) + EPSILON)
    normed = (floats * inv_rms * (1.0 + layer_gain.astype(jnp.float32))[None, :]).astype(jnp.bfloat16)
    projected = jnp.dot(normed, layer_weight, preferred_element_type=jnp.float32)
    query_cols = QHEADS * HEAD
    key_cols = KVHEADS * HEAD
    query_states = rotate(projected[:, :query_cols], positions, QHEADS).astype(jnp.bfloat16)
    key_states = rotate(projected[:, query_cols:query_cols + key_cols], positions, KVHEADS).astype(jnp.bfloat16)
    value_states = projected[:, query_cols + key_cols:].astype(jnp.bfloat16)
    return (query_states, key_states, value_states, new_weight, new_gain)
```

```python
import functools
import heapq

import jax
import jax.numpy as jnp
from jax import lax
from jax.experimental import pallas as pl
from jax.experimental.pallas import tpu as pltpu
from jax.sharding import PartitionSpec as P

HEAD = 256
EPSILON = 1e-06
ADVANCE_RATE = 0.5
ROPE_BASE = 10000.0
MESH = pl.DeviceIdType.MESH

RINGS = {"x": 4, "y": 4, "z": 8}
BLOCKS = 128
ROWS = 112
COLS = 512
TOK = 480
WIDTH = 3584
ROUTES = (("xyz", 0, 16), ("yzx", 16, 64), ("xzy", 64, 112))
ROUTE_ORDER = (1, 2, 0)


def reach(ring, sign, parity):
    return ring // 2 if (sign > 0) == (parity % 2 == 0) else ring // 2 - 1


def plan():
    rate, latency = 46.6e3, 2.2
    busy, queue, steps, ids = {}, [], [], {}
    serial = 0

    def push(at, event):
        nonlocal serial
        heapq.heappush(queue, (at, serial, event))
        serial += 1

    def send(at, route, item, axis, sign, outs):
        order, low, high = ROUTES[route]
        size = (high - low) * COLS * 2 * (1 if item[0] == 1 else RINGS[order[0]])
        begin = max(at, busy.get((axis, sign), 0.0))
        busy[axis, sign] = begin + size / rate
        ids[route, item] = len(ids)
        outs.append((item, axis, sign))
        push(busy[axis, sign] + latency, ("item", route, item, sign))

    at = 10.0
    for route in ROUTE_ORDER:
        at += (ROUTES[route][2] - ROUTES[route][1]) / ROWS * 9.8
        push(at, ("own", route, None, 0))
    left = {}
    while queue:
        at, _, (kind, route, item, sign) = heapq.heappop(queue)
        one, two, three = ROUTES[route][0]
        outs = []
        if kind == "own":
            left[route] = RINGS[one] - 1
            for s in (1, -1):
                if reach(RINGS[one], s, route):
                    send(at, route, (1, s, 0), one, s, outs)
        elif item[0] == 1:
            if abs(item[1]) < reach(RINGS[one], sign, route):
                send(at, route, (1, item[1] + sign, 0), one, sign, outs)
            left[route] -= 1
            if left[route] == 0:
                for s in (1, -1):
                    send(at, route, (2, s, 0), two, s, outs)
                for s in (1, -1):
                    send(at, route, (3, 0, s), three, s, outs)
        elif item[0] == 2:
            if abs(item[1]) < reach(RINGS[two], sign, route + 1):
                send(at, route, (2, item[1] + sign, 0), two, sign, outs)
            for s in (1, -1):
                send(at, route, (3, item[1], s), three, s, outs)
        else:
            if abs(item[2]) < reach(RINGS[three], sign, item[1]):
                send(at, route, (3, item[1], item[2] + sign), three, sign, outs)
        steps.append((kind, route, item, outs))
    return steps, ids


def kernel(
    steps, ids,
    tok_in, fast_in, slow_in, gain_in, cos_in, sin_in,
    q_out, k_out, v_out, weight_out, gain_out,
    buf0, buf1, buf2, tok, own1, got1, sum2, got2, slow, fresh, gain, gain_got1, gain_sum, gain_got2, gain_new,
    cosine, sine, turn_c, turn_s, acc, out,
    load_sem, pair_send, pair_recv, rs_send, rs_recv, item_recv, item_send, hand_send, hand_recv, out_sem,
):
    bufs = (buf0, buf1, buf2)
    f = lax.axis_index("fsdp")
    r = lax.axis_index("rep")
    zl, x, y = lax.rem(f, 2), lax.rem(f // 2, 4), f // 8
    zh, c = r // 2, lax.rem(r, 2)
    z = zh * 2 + zl
    at = {"x": x, "y": y, "z": z}

    def device(px, py, pz, pc):
        return ((py * 4 + px) * 2 + lax.rem(pz, 2), (pz // 2) * 2 + pc)

    def wrap(p, off, n):
        return lax.rem(p + (off % n), n)

    def beside(axis, sign):
        p = dict(at)
        p[axis] = wrap(p[axis], sign, RINGS[axis])
        return device(p["x"], p["y"], p["z"], c)

    partner = (f, zh * 2 + 1 - c)
    peers = [(f, wrap(zh, k, 4) * 2 + c) for k in (1, 2, 3)]
    sides = {(a, s): beside(a, s) for a in "xyz" for s in (1, -1)}

    def load(src, dst, sem):
        return pltpu.make_async_copy(src, dst, load_sem.at[sem])

    loads = [
        load(gain_in, gain, 0),
        load(slow_in, slow, 1),
        load(tok_in, tok, 2),
        load(cos_in, cosine, 3),
        load(sin_in, sine, 4),
    ]
    mine = []
    for k in range(4):
        cols = pl.ds(pl.multiple_of((k * 2 + c) * COLS, COLS), COLS)
        mine.append(load(fast_in.at[:, cols], own1.at[k], 5 + k))
    for copy in mine + loads:
        copy.start()

    barrier = pltpu.get_barrier_semaphore()
    everyone = [partner] + peers + list(sides.values())
    for peer in everyone:
        pl.semaphore_signal(barrier, inc=1, device_id=peer, device_id_type=MESH)
    pl.semaphore_wait(barrier, len(everyone))

    def remote(src, dst, send_sem, recv_sem, peer):
        return pltpu.make_async_remote_copy(
            src_ref=src, dst_ref=dst, send_sem=send_sem, recv_sem=recv_sem,
            device_id=peer, device_id_type=MESH,
        )

    pair = []
    for k in range(4):
        cols = pl.ds(pl.multiple_of((k * 2 + 1 - c) * COLS, COLS), COLS)
        pair.append(remote(fast_in.at[:, cols], got1.at[k], pair_send.at[k], pair_recv.at[k], partner))
    loads[0].wait()
    pair.append(remote(gain, gain_got1, pair_send.at[4], pair_recv.at[4], partner))
    for copy in pair:
        copy.start()
    for copy in mine:
        copy.wait()
    for copy in pair:
        copy.wait_recv()
    gain_sum[...] = gain[...] + gain_got1[...]
    for k in (1, 2, 3):
        to = wrap(zh, k, 4)
        sum2[k - 1] = (own1[to].astype(jnp.float32) + got1[to].astype(jnp.float32)).astype(jnp.bfloat16)
    scatter = []
    for n in range(3):
        scatter.append(remote(gain_sum, gain_got2.at[n], rs_send.at[9 + n], rs_recv.at[9 + n], peers[n]))
    for route in ROUTE_ORDER:
        rows = pl.ds(ROUTES[route][1], ROUTES[route][2] - ROUTES[route][1])
        for n in range(3):
            s = route * 3 + n
            scatter.append(
                remote(sum2.at[n, rows], got2.at[n, rows], rs_send.at[s], rs_recv.at[s], peers[n])
            )
    for copy in scatter:
        copy.start()
    loads[1].wait()
    for copy in scatter[:3]:
        copy.wait_recv()
    totals = gain_sum[...] + gain_got2[0] + gain_got2[1] + gain_got2[2]
    old_gain = totals[1:2, :]
    new_gain = old_gain + ADVANCE_RATE * (totals[0:1, :] / 8.0 - old_gain)
    gain_new[...] = jnp.broadcast_to(new_gain, (8, 128))
    scale_row = 1.0 + new_gain.astype(jnp.bfloat16).astype(jnp.float32)
    gain_store = pltpu.make_async_copy(gain_new, gain_out, out_sem.at[8])
    gain_store.start()

    def update(route):
        low, high = ROUTES[route][1:]
        for n in range(3):
            rows = pl.ds(low, high - low)
            remote(
                sum2.at[n, rows], got2.at[n, rows], rs_send.at[route * 3 + n], rs_recv.at[route * 3 + n], peers[n]
            ).wait_recv()
        total = own1[zh, low:high].astype(jnp.float32) + got1[zh, low:high].astype(jnp.float32)
        for n in range(3):
            total = total + got2[n, low:high].astype(jnp.float32)
        old = slow[low:high]
        new = old + ADVANCE_RATE * (total / 8.0 - old)
        fresh[low:high] = new
        shape = (high - low, 128)
        eye = lax.broadcasted_iota(jnp.int32, shape, 0) + low == lax.broadcasted_iota(jnp.int32, shape, 1)
        scale = jnp.sum(jnp.where(eye, jnp.broadcast_to(scale_row, shape), 0.0), axis=1, keepdims=True)
        scaled = new.astype(jnp.bfloat16).astype(jnp.float32) * scale
        bufs[route][c, piece(route, (1, 0, 0))[0]] = scaled.astype(jnp.bfloat16)

    def piece(route, item):
        one, two, three = ROUTES[route][0]
        n1, n2, n3 = RINGS[one], RINGS[two], RINGS[three]
        p1, p2, p3 = at[one], at[two], at[three]
        if item[0] == 1:
            return (p3 * n2 + p2) * n1 + wrap(p1, -item[1], n1), 1
        if item[0] == 2:
            return (p3 * n2 + wrap(p2, -item[1], n2)) * n1, n1
        return (wrap(p3, -item[2], n3) * n2 + wrap(p2, -item[1], n2)) * n1, n1

    def view(route, item):
        start, size = piece(route, item)
        return bufs[route].at[c, pl.ds(start, size)]

    def forward(route, item, axis, sign):
        phase, a, b = item
        held = (phase, a - sign, b) if phase < 3 else (phase, a, b - sign)
        part = view(route, held)
        remote(part, part, item_send.at[route], item_recv.at[ids[route, item]], sides[axis, sign]).start()

    def hand(route, item):
        part = view(route, item)
        remote(part, part, hand_send.at[route], hand_recv.at[route], partner).start()

    def tables():
        loads[2].wait()
        loads[3].wait()
        loads[4].wait()

        def rows_of(i, _):
            rows = pl.ds(pl.multiple_of(i * 16, 16), 16)
            t = tok[rows, :].astype(jnp.float32)
            inv = lax.rsqrt(jnp.sum(t * t, axis=1, keepdims=True) * (1.0 / WIDTH) + EPSILON)
            turn_c[0, rows, :] = cosine[rows, :] * inv
            turn_s[0, rows, :] = sine[rows, :] * inv
            turn_c[1, rows, :] = jnp.broadcast_to(inv, (16, 128))
            turn_s[1, rows, :] = jnp.zeros((16, 128), jnp.float32)
            return 0

        lax.fori_loop(0, TOK // 16, rows_of, 0)

    started = 0
    for kind, route, item, outs in steps:
        if kind == "own":
            update(route)
            item = (1, 0, 0)
        else:
            part = view(route, item)
            remote(part, part, item_send.at[route], item_recv.at[ids[route, item]], partner).wait_recv()
        for target, axis, sign in outs:
            forward(route, target, axis, sign)
        hand(route, item)
        if kind == "own":
            started += 1
            if started == 3:
                weight_store = pltpu.make_async_copy(fresh, weight_out, out_sem.at[9])
                weight_store.start()
                tables()

    for route in range(3):
        other = bufs[route].at[1 - c]
        remote(other, other, hand_send.at[route], hand_recv.at[route], partner).wait_recv()

    def columns(b, _):
        bz, bc = b // 2, lax.rem(b, 2)
        parts = []
        for py in range(4):
            for px in range(4):
                for pz in range(2):
                    wz = bz * 2 + pz
                    parts.append(buf0[bc, (wz * 4 + py) * 4 + px])
                    parts.append(buf1[bc, (px * 8 + wz) * 4 + py])
                    parts.append(buf2[bc, (py * 8 + wz) * 4 + px])
        acc[...] = jnp.dot(tok[...], jnp.concatenate(parts, axis=0), preferred_element_type=jnp.float32)
        kind = b // 6
        for h in range(0, COLS, HEAD):
            u, w = acc[:, h : h + 128], acc[:, h + 128 : h + 256]
            tc, ts = turn_c[kind], turn_s[kind]
            out[b, :, h : h + 128] = (u * tc - w * ts).astype(jnp.bfloat16)
            out[b, :, h + 128 : h + 256] = (w * tc + u * ts).astype(jnp.bfloat16)

        def put(ref, first):
            cols = pl.ds(pl.multiple_of((b - first) * COLS, COLS), COLS)
            pltpu.make_async_copy(out.at[b], ref.at[:, cols], out_sem.at[b]).start()

        @pl.when(b < 4)
        def _():
            put(q_out, 0)

        @pl.when((b >= 4) & (b < 6))
        def _():
            put(k_out, 4)

        @pl.when(b >= 6)
        def _():
            put(v_out, 6)

        return 0

    lax.fori_loop(0, 8, columns, 0)

    for copy in pair + scatter:
        copy.wait_send()
    for route in range(3):
        most = bufs[route].at[0, pl.ds(0, BLOCKS - 1)]
        remote(most, most, item_send.at[route], item_recv.at[0], partner).wait_send()
        every = bufs[route].at[0]
        remote(every, every, hand_send.at[route], hand_recv.at[route], partner).wait_send()
    gain_store.wait()
    weight_store.wait()
    for b in range(8):
        ref, first = ((q_out, 0), (k_out, 4), (v_out, 6))[(b >= 4) + (b >= 6)]
        pltpu.make_async_copy(out.at[b], ref.at[:, pl.ds((b - first) * COLS, COLS)], out_sem.at[b]).wait()


def on_device(tokens, positions, slow_weight, fast_weight, slow_gain, fast_gain):
    steps, ids = plan()
    r = lax.axis_index("rep")
    half = HEAD // 2
    rates = ROPE_BASE ** (-(jnp.arange(half, dtype=jnp.float32) * 2.0 / HEAD))
    angles = positions.astype(jnp.float32)[:, None] * rates[None, :]
    placed = lax.dynamic_update_slice(jnp.zeros((128,), jnp.float32), slow_gain, (r * 14,))
    fast_row = jnp.pad(fast_gain.astype(jnp.float32), ((0, 0), (0, 128 - ROWS)))
    gains = jnp.concatenate([fast_row, placed[None], jnp.zeros((6, 128), jnp.float32)], axis=0)
    f32, bf16 = jnp.float32, jnp.bfloat16
    vmem, dma = pltpu.VMEM, pltpu.SemaphoreType.DMA
    anywhere = pl.BlockSpec(memory_space=pl.ANY)
    q, k, v, new_weight, new_gain = pl.pallas_call(
        functools.partial(kernel, steps, ids),
        out_shape=(
            jax.ShapeDtypeStruct((TOK, 2048), bf16),
            jax.ShapeDtypeStruct((TOK, 1024), bf16),
            jax.ShapeDtypeStruct((TOK, 1024), bf16),
            jax.ShapeDtypeStruct((ROWS, COLS), f32),
            jax.ShapeDtypeStruct((8, 128), f32),
        ),
        in_specs=[anywhere] * 6,
        out_specs=(anywhere,) * 5,
        scratch_shapes=[
            *(vmem((2, BLOCKS, high - low, COLS), bf16) for _, low, high in ROUTES),
            vmem((TOK, WIDTH), bf16),
            vmem((4, ROWS, COLS), bf16),
            vmem((4, ROWS, COLS), bf16),
            vmem((3, ROWS, COLS), bf16),
            vmem((3, ROWS, COLS), bf16),
            vmem((ROWS, COLS), f32),
            vmem((ROWS, COLS), f32),
            vmem((8, 128), f32),
            vmem((8, 128), f32),
            vmem((8, 128), f32),
            vmem((3, 8, 128), f32),
            vmem((8, 128), f32),
            vmem((TOK, 128), f32),
            vmem((TOK, 128), f32),
            vmem((2, TOK, 128), f32),
            vmem((2, TOK, 128), f32),
            vmem((TOK, COLS), f32),
            vmem((8, TOK, COLS), bf16),
            dma((9,)),
            dma((5,)),
            dma((5,)),
            dma((12,)),
            dma((12,)),
            dma((len(ids),)),
            dma((3,)),
            dma((3,)),
            dma((3,)),
            dma((10,)),
        ],
        compiler_params=pltpu.CompilerParams(
            collective_id=0, has_side_effects=True, vmem_limit_bytes=60 * 1024 * 1024
        ),
    )(tokens, fast_weight[0], slow_weight, gains, jnp.cos(angles), jnp.sin(angles))
    return q, k, v, new_weight, lax.dynamic_slice(new_gain[0], (r * 14,), (14,))


def solution(mesh):
    return jax.shard_map(
        on_device,
        mesh=mesh,
        in_specs=(
            P(("fsdp", "rep"), None),
            P(("fsdp", "rep")),
            P("fsdp", "rep"),
            P("rep", "fsdp", None),
            P(("fsdp", "rep")),
            P("rep", "fsdp"),
        ),
        out_specs=(
            P(("fsdp", "rep"), None),
            P(("fsdp", "rep"), None),
            P(("fsdp", "rep"), None),
            P("fsdp", "rep"),
            P(("fsdp", "rep")),
        ),
        check_vma=False,
    )
```

```python
import functools
import heapq

import jax
import jax.numpy as jnp
from jax import lax
from jax.experimental import pallas as pl
from jax.experimental.pallas import tpu as pltpu
from jax.sharding import PartitionSpec as P

HEAD = 256
EPSILON = 1e-06
ADVANCE_RATE = 0.5
LOG_BASE = 9.210340371976184
MESH = pl.DeviceIdType.MESH

RINGS = {"x": 4, "y": 4, "z": 8}
BLOCKS = 128
ROWS = 112
COLS = 512
TOK = 480
WIDTH = 3584
ROUTES = (("xyz", 0, 16), ("yzx", 16, 32), ("yzx", 32, 64), ("xzy", 64, 80), ("xzy", 80, 112))
ROUTE_ORDER = (3, 1, 4, 2, 0)
NR = len(ROUTES)
GROUPS = ((1, 3), (0, 2, 4))
HAND_TIME = 2.5
HALF_K = WIDTH // 2
STRIPS = ((0, 0, 2), (1, 0, 2), (2, 0, 1), (2, 1, 1), (3, 0, 2), (4, 0, 1), (4, 1, 1))
TABLE_ROWS = ((0, 128), (128, 128), (256, 128), (384, 96))


def reach(ring, sign, parity):
    return ring // 2 if (sign > 0) == (parity % 2 == 0) else ring // 2 - 1


def distance(route, item):
    place = ROUTES[route][0].index("z")
    if item[0] <= place:
        return 0
    return item[place] % 8


def plan():
    rate, latency = 46.6e3, 2.2
    busy, queue, events, ids = {}, [], [], {}
    serial = 0

    def push(at, event):
        nonlocal serial
        heapq.heappush(queue, (at, serial, event))
        serial += 1

    def send(at, route, item, axis, sign, outs):
        order, low, high = ROUTES[route]
        size = (high - low) * COLS * 2 * (1 if item[0] == 1 else RINGS[order[0]])
        begin = max(at, busy.get((axis, sign), 0.0))
        busy[axis, sign] = begin + size / rate
        ids[route, item] = len(ids)
        outs.append((item, axis, sign))
        push(busy[axis, sign] + latency, ("item", route, item, sign))

    at = 10.0
    for route in ROUTE_ORDER:
        at += (ROUTES[route][2] - ROUTES[route][1]) / ROWS * 9.8
        push(at, ("own", route, None, 0))
    left = {}
    ready = {}
    while queue:
        at, _, (kind, route, item, sign) = heapq.heappop(queue)
        one, two, three = ROUTES[route][0]
        outs = []
        if kind == "own":
            left[route] = RINGS[one] - 1
            for s in (1, -1):
                if reach(RINGS[one], s, route):
                    send(at, route, (1, s, 0), one, s, outs)
        elif item[0] == 1:
            if abs(item[1]) < reach(RINGS[one], sign, route):
                send(at, route, (1, item[1] + sign, 0), one, sign, outs)
            left[route] -= 1
            if left[route] == 0:
                for s in (1, -1):
                    send(at, route, (2, s, 0), two, s, outs)
                for s in (1, -1):
                    send(at, route, (3, 0, s), three, s, outs)
        elif item[0] == 2:
            if abs(item[1]) < reach(RINGS[two], sign, route + 1):
                send(at, route, (2, item[1] + sign, 0), two, sign, outs)
            for s in (1, -1):
                send(at, route, (3, item[1], s), three, s, outs)
        else:
            if abs(item[2]) < reach(RINGS[three], sign, item[1]):
                send(at, route, (3, item[1], item[2] + sign), three, sign, outs)
        z = distance(route, item or (1, 0, 0))
        ready[route, z] = at
        events.append((at, (kind, route, item, outs)))

    fill = [("strip", n, 1.2) for n in range(len(STRIPS))]
    fill += [("table", n, 0.8) for n in range(len(TABLE_ROWS))]
    units = sorted((max(ready[route, z] for route in group), group, z) for group in GROUPS for z in range(8))
    ends = {}
    for far, need in ((0, (0, 1, 7)), (1, (1, 2, 3)), (3, (5, 6, 7)), (2, (3, 4, 5))):
        ends.setdefault(max(n for n, u in enumerate(units) if u[2] in need), []).append(far)
    work = []
    for n, (when, group, z) in enumerate(units):
        work.append((("unit", group, z), 0.5 * len(group), when))
        work += [(("finish", far), 0.8, when) for far in ends.get(n, ())]
    steps = []
    clock = 8.5
    for at, event in events:
        while fill and at - clock >= 0.6 * fill[0][2]:
            steps.append(fill[0][:2])
            clock += fill.pop(0)[2]
        while work and not fill and work[0][2] < at and work[0][2] + HAND_TIME <= max(clock, at):
            steps.append(work[0][0])
            clock = max(clock, work[0][2] + HAND_TIME) + work.pop(0)[1]
        clock = max(clock, at) + 0.12
        steps.append(event)
    steps += [entry[:2] for entry in fill] + [entry[0] for entry in work]
    return steps, ids


def kernel(
    steps, ids,
    tok_in, fast_in, slow_in, fast_gain_in, slow_gain_in, pos_in,
    q_out, k_out, v_out, weight_out, gain_out,
    *rest,
):
    bufs, rest = rest[:NR], rest[NR:]
    (
        tok, perm, strips, acc, own1, got1, sum2, got2, slow, fast_gain, slow_gain, pos,
        gain, gain_got1, gain_sum, gain_got2, gain_new, turn_c, turn_s, scale,
        load_sem, pair_send, pair_recv, rs_send, rs_recv, item_recv, item_send, hand_send, hand_recv,
    ) = rest
    f = lax.axis_index("fsdp")
    r = lax.axis_index("rep")
    zl, x, y = lax.rem(f, 2), lax.rem(f // 2, 4), f // 8
    zh, c = r // 2, lax.rem(r, 2)
    z = zh * 2 + zl
    at = {"x": x, "y": y, "z": z}

    def device(px, py, pz, pc):
        return ((py * 4 + px) * 2 + lax.rem(pz, 2), (pz // 2) * 2 + pc)

    def wrap(p, off, n):
        return lax.rem(p + (off % n), n)

    def beside(axis, sign):
        p = dict(at)
        p[axis] = wrap(p[axis], sign, RINGS[axis])
        return device(p["x"], p["y"], p["z"], c)

    partner = (f, zh * 2 + 1 - c)
    peers = [(f, wrap(zh, k, 4) * 2 + c) for k in (1, 2, 3)]
    sides = {(a, s): beside(a, s) for a in "xyz" for s in (1, -1)}

    def load(src, dst, sem):
        return pltpu.make_async_copy(src, dst, load_sem.at[sem])

    loads = [
        load(fast_gain_in, fast_gain, 0),
        load(slow_gain_in, slow_gain.at[0:1], 1),
        load(slow_in, slow, 2),
        load(pos_in, pos, 3),
        load(tok_in, tok, 4),
    ]
    mine = []
    for k in range(4):
        cols = pl.ds(pl.multiple_of((k * 2 + c) * COLS, COLS), COLS)
        mine.append(load(fast_in.at[:, cols], own1.at[k], 5 + k))
    barrier = pltpu.get_barrier_semaphore()
    everyone = [partner] + peers + list(sides.values())
    for peer in everyone:
        pl.semaphore_signal(barrier, inc=1, device_id=peer, device_id_type=MESH)
    for copy in loads[:2] + mine + loads[2:]:
        copy.start()

    def clear(b, _):
        acc[b] = jnp.zeros((TOK, COLS), jnp.float32)
        return 0

    lax.fori_loop(0, 8, clear, 0)
    for copy in loads[:2]:
        copy.wait()
    lanes = lax.broadcasted_iota(jnp.int32, (8, 128), 1)
    gain[...] = jnp.where(lanes < 14, slow_gain[...], 0.0)
    gain[...] = pltpu.roll(gain[...], r * 14, 1)
    gain[1:2, :] = gain[0:1, :]
    gain[0:1, :] = jnp.zeros((1, 128), jnp.float32)
    gain[0:1, 0:ROWS] = fast_gain[...].astype(jnp.float32)
    pl.semaphore_wait(barrier, len(everyone))

    def remote(src, dst, send_sem, recv_sem, peer):
        return pltpu.make_async_remote_copy(
            src_ref=src, dst_ref=dst, send_sem=send_sem, recv_sem=recv_sem,
            device_id=peer, device_id_type=MESH,
        )

    pair = []
    for k in range(4):
        cols = pl.ds(pl.multiple_of((k * 2 + 1 - c) * COLS, COLS), COLS)
        pair.append(remote(fast_in.at[:, cols], got1.at[k], pair_send.at[k], pair_recv.at[k], partner))
    pair.append(remote(gain, gain_got1, pair_send.at[4], pair_recv.at[4], partner))
    for copy in pair:
        copy.start()
    for copy in mine:
        copy.wait()
    for copy in pair:
        copy.wait_recv()
    gain_sum[...] = gain[...] + gain_got1[...]
    for k in (1, 2, 3):
        to = wrap(zh, k, 4)
        sum2[k - 1] = (own1[to].astype(jnp.float32) + got1[to].astype(jnp.float32)).astype(jnp.bfloat16)
    scatter = []
    for n in range(3):
        s = NR * 3 + n
        scatter.append(remote(gain_sum, gain_got2.at[n], rs_send.at[s], rs_recv.at[s], peers[n]))
    for route in ROUTE_ORDER:
        rows = pl.ds(ROUTES[route][1], ROUTES[route][2] - ROUTES[route][1])
        for n in range(3):
            s = route * 3 + n
            scatter.append(
                remote(sum2.at[n, rows], got2.at[n, rows], rs_send.at[s], rs_recv.at[s], peers[n])
            )
    for copy in scatter:
        copy.start()

    def gains():
        loads[2].wait()
        for copy in scatter[:3]:
            copy.wait_recv()
        totals = gain_sum[...] + gain_got2[0] + gain_got2[1] + gain_got2[2]
        old_gain = totals[1:2, :]
        new_gain = old_gain + ADVANCE_RATE * (totals[0:1, :] / 8.0 - old_gain)
        row = 1.0 + new_gain.astype(jnp.bfloat16).astype(jnp.float32)
        eye = lax.broadcasted_iota(jnp.int32, (ROWS, 128), 0) == lax.broadcasted_iota(jnp.int32, (ROWS, 128), 1)
        column = jnp.sum(jnp.where(eye, jnp.broadcast_to(row, (ROWS, 128)), 0.0), axis=1, keepdims=True)
        scale[...] = jnp.broadcast_to(column, (ROWS, 128))
        gain_new[...] = jnp.broadcast_to(new_gain, (8, 128))
        gain_new[...] = pltpu.roll(gain_new[...], lax.rem(128 - r * 14, 128), 1)
        gain_out[...] = gain_new[0:1, 0:14]

    def update(route):
        low, high = ROUTES[route][1:]
        for n in range(3):
            rows = pl.ds(low, high - low)
            remote(
                sum2.at[n, rows], got2.at[n, rows], rs_send.at[route * 3 + n], rs_recv.at[route * 3 + n], peers[n]
            ).wait_recv()
        total = own1[zh, low:high].astype(jnp.float32) + got1[zh, low:high].astype(jnp.float32)
        for n in range(3):
            total = total + got2[n, low:high].astype(jnp.float32)
        old = slow[low:high]
        new = old + ADVANCE_RATE * (total / 8.0 - old)
        weight_out[low:high] = new
        scaled = new.astype(jnp.bfloat16).astype(jnp.float32) * jnp.tile(scale[low:high], (1, COLS // 128))
        bufs[route][c, piece(route, (1, 0, 0))[0]] = scaled.astype(jnp.bfloat16)

    def spot(route, px, py, pz):
        one, two, three = ROUTES[route][0]
        p = {"x": px, "y": py, "z": pz}
        return (p[three] * RINGS[two] + p[two]) * RINGS[one] + p[one]

    def piece(route, item):
        one, two, three = ROUTES[route][0]
        n1, n2, n3 = RINGS[one], RINGS[two], RINGS[three]
        p1, p2, p3 = at[one], at[two], at[three]
        if item[0] == 1:
            return (p3 * n2 + p2) * n1 + wrap(p1, -item[1], n1), 1
        if item[0] == 2:
            return (p3 * n2 + wrap(p2, -item[1], n2)) * n1, n1
        return (wrap(p3, -item[2], n3) * n2 + wrap(p2, -item[1], n2)) * n1, n1

    def view(route, item):
        start, size = piece(route, item)
        return bufs[route].at[c, pl.ds(start, size)]

    def forward(route, item, axis, sign):
        phase, a, b = item
        held = (phase, a - sign, b) if phase < 3 else (phase, a, b - sign)
        part = view(route, held)
        remote(part, part, item_send.at[route], item_recv.at[ids[route, item]], sides[axis, sign]).start()

    def hand(route, item):
        part = view(route, item)
        sem = hand_recv.at[route * 8 + distance(route, item)]
        remote(part, part, hand_send.at[route], sem, partner).start()

    def table(first, count):
        rows = pl.ds(first, count)
        spots = jnp.broadcast_to(pos[0:1, first : first + count].astype(jnp.float32), (count, count))
        eye = lax.broadcasted_iota(jnp.int32, (count, count), 0) == lax.broadcasted_iota(jnp.int32, (count, count), 1)
        place = jnp.sum(jnp.where(eye, spots, 0.0), axis=1, keepdims=True)
        lane = lax.broadcasted_iota(jnp.int32, (1, 128), 1).astype(jnp.float32)
        rates = jnp.exp(lane * (-2.0 / HEAD * LOG_BASE))
        angles = place * rates
        t = tok[rows, :].astype(jnp.float32)
        inv = lax.rsqrt(jnp.sum(t * t, axis=1, keepdims=True) * (1.0 / WIDTH) + EPSILON)
        turn_c[0, rows, :] = jnp.cos(angles) * inv
        turn_s[rows, :] = jnp.sin(angles) * inv
        turn_c[1, rows, :] = jnp.broadcast_to(inv, (count, 128))

    def strip(n):
        route, parity, parities = STRIPS[n]
        low, high = ROUTES[route][1:]
        tall = high - low
        lane = lax.broadcasted_iota(jnp.int32, (1, 256), 1)
        if parities == 2:
            pz, lane = lane // 128, lax.rem(lane, 128)
        else:
            pz = parity
        source = (lane // tall) * (2 * ROWS) + pz * ROWS + low + lax.rem(lane, tall)

        def rows_of(i, _):
            first = pl.multiple_of(i * 128, 128)
            k = lax.broadcasted_iota(jnp.int32, (128, 256), 0) + first
            perm[pl.ds(first, 128), :] = jnp.where(k == source, 1.0, 0.0).astype(jnp.bfloat16)
            return 0

        lax.fori_loop(0, HALF_K // 128, rows_of, 0)
        for p in range(2):
            moved = jnp.dot(
                tok[:, HALF_K * p : HALF_K * (p + 1)], perm[...], preferred_element_type=jnp.float32
            ).astype(jnp.bfloat16)
            to = 16 * low + p * 8 * tall
            if parities == 2:
                strips[0, :, to : to + 128] = moved[:, :128]
                strips[1, :, to : to + 128] = moved[:, 128:]
            else:
                strips[parity, :, to : to + 256] = moved

    def unit(group, far):
        for route in group:
            some = bufs[route].at[1 - c, pl.ds(0, 16)]
            remote(some, some, hand_send.at[route], hand_recv.at[route * 8 + far], partner).wait_recv()
        wz = wrap(z, -far, 8)

        def of_core(bc, _):
            parts = [
                bufs[route][bc, spot(route, px, py, wz)] for route in group for py in range(4) for px in range(4)
            ]
            lanes = [
                strips[lax.rem(wz, 2), :, 16 * ROUTES[route][1] : 16 * ROUTES[route][2]] for route in group
            ]
            acc[(wz // 2) * 2 + bc] += jnp.dot(
                jnp.concatenate(lanes, axis=1), jnp.concatenate(parts, axis=0), preferred_element_type=jnp.float32
            )
            return 0

        lax.fori_loop(0, 2, of_core, 0)

    def finish(far):
        bz = wrap(zh, -far, 4)

        def of_core(bc, _):
            b = bz * 2 + bc

            def turned(ref, first):
                start = (b - first) * COLS
                for h in range(0, COLS, HEAD):
                    u, w = acc[b, :, h : h + 128], acc[b, :, h + 128 : h + 256]
                    tc, ts = turn_c[0], turn_s[...]
                    ref[:, pl.ds(pl.multiple_of(start + h, 128), 128)] = (u * tc - w * ts).astype(jnp.bfloat16)
                    ref[:, pl.ds(pl.multiple_of(start + h + 128, 128), 128)] = (w * tc + u * ts).astype(jnp.bfloat16)

            @pl.when(b < 4)
            def _():
                turned(q_out, 0)

            @pl.when((b >= 4) & (b < 6))
            def _():
                turned(k_out, 4)

            @pl.when(b >= 6)
            def _():
                for h in range(0, COLS, 128):
                    cols = pl.ds(pl.multiple_of((b - 6) * COLS + h, 128), 128)
                    v_out[:, cols] = (acc[b, :, h : h + 128] * turn_c[1]).astype(jnp.bfloat16)

            return 0

        lax.fori_loop(0, 2, of_core, 0)

    first_strip, first_table, first_own = True, True, True
    for step in steps:
        if step[0] == "strip":
            if first_strip:
                loads[4].wait()
                first_strip = False
            strip(step[1])
        elif step[0] == "table":
            if first_table:
                loads[3].wait()
                first_table = False
            table(*TABLE_ROWS[step[1]])
        elif step[0] == "unit":
            unit(*step[1:])
        elif step[0] == "finish":
            finish(step[1])
        else:
            kind, route, item, outs = step
            if kind == "own":
                if first_own:
                    gains()
                    first_own = False
                update(route)
                item = (1, 0, 0)
            else:
                part = view(route, item)
                remote(part, part, item_send.at[route], item_recv.at[ids[route, item]], partner).wait_recv()
            for target, axis, sign in outs:
                forward(route, target, axis, sign)
            hand(route, item)

    for copy in pair + scatter:
        copy.wait_send()
    for route in range(NR):
        most = bufs[route].at[0, pl.ds(0, BLOCKS - 1)]
        remote(most, most, item_send.at[route], item_recv.at[0], partner).wait_send()
        every = bufs[route].at[0]
        remote(every, every, hand_send.at[route], hand_recv.at[0], partner).wait_send()


def flush(*refs):
    sem = refs[-1]
    count = len(refs) // 2
    copies = [pltpu.make_async_copy(refs[n], refs[count + n], sem.at[n]) for n in range(count)]
    for copy in copies:
        copy.start()
    for copy in copies:
        copy.wait()


def on_device(tokens, positions, slow_weight, fast_weight, slow_gain, fast_gain):
    steps, ids = plan()
    f32, bf16 = jnp.float32, jnp.bfloat16
    vmem, dma = pltpu.VMEM, pltpu.SemaphoreType.DMA
    shapes = (
        ((TOK, 2048), bf16),
        ((TOK, 1024), bf16),
        ((TOK, 1024), bf16),
        ((ROWS, COLS), f32),
        ((1, 14), f32),
    )
    held = pl.BlockSpec(memory_space=pltpu.VMEM)
    far = pl.BlockSpec(memory_space=pltpu.HBM)
    results = pl.pallas_call(
        functools.partial(kernel, steps, ids),
        out_shape=tuple(vmem(*s) for s in shapes),
        in_specs=[far] * 6,
        out_specs=(held,) * 5,
        scratch_shapes=[
            *(vmem((2, BLOCKS, high - low, COLS), bf16) for _, low, high in ROUTES),
            vmem((TOK, WIDTH), bf16),
            vmem((HALF_K, 256), bf16),
            vmem((2, TOK, HALF_K), bf16),
            vmem((8, TOK, COLS), f32),
            vmem((4, ROWS, COLS), bf16),
            vmem((4, ROWS, COLS), bf16),
            vmem((3, ROWS, COLS), bf16),
            vmem((3, ROWS, COLS), bf16),
            vmem((ROWS, COLS), f32),
            vmem((1, ROWS), bf16),
            vmem((8, 128), f32),
            vmem((1, TOK), jnp.int32),
            vmem((8, 128), f32),
            vmem((8, 128), f32),
            vmem((8, 128), f32),
            vmem((3, 8, 128), f32),
            vmem((8, 128), f32),
            vmem((2, TOK, 128), f32),
            vmem((TOK, 128), f32),
            vmem((ROWS, 128), f32),
            dma((9,)),
            dma((5,)),
            dma((5,)),
            dma((NR * 3 + 3,)),
            dma((NR * 3 + 3,)),
            dma((len(ids),)),
            dma((NR,)),
            dma((NR,)),
            dma((NR * 8,)),
        ],
        compiler_params=pltpu.CompilerParams(
            collective_id=0, has_side_effects=True, vmem_limit_bytes=57 * 1024 * 1024
        ),
    )(
        tokens, fast_weight[0], slow_weight, fast_gain,
        jnp.pad(slow_gain.reshape(1, 14), ((0, 0), (0, 114))), positions.reshape(1, TOK),
    )
    q, k, v, new_weight, new_gain = pl.pallas_call(
        flush,
        out_shape=tuple(jax.ShapeDtypeStruct(*s) for s in shapes),
        in_specs=[held] * 5,
        out_specs=(far,) * 5,
        scratch_shapes=[dma((5,))],
        compiler_params=pltpu.CompilerParams(vmem_limit_bytes=1024 * 1024),
    )(*results)
    return q, k, v, new_weight, new_gain.reshape(14)


def solution(mesh):
    return jax.shard_map(
        on_device,
        mesh=mesh,
        in_specs=(
            P(("fsdp", "rep"), None),
            P(("fsdp", "rep")),
            P("fsdp", "rep"),
            P("rep", "fsdp", None),
            P(("fsdp", "rep")),
            P("rep", "fsdp"),
        ),
        out_specs=(
            P(("fsdp", "rep"), None),
            P(("fsdp", "rep"), None),
            P(("fsdp", "rep"), None),
            P("fsdp", "rep"),
            P(("fsdp", "rep")),
        ),
        check_vma=False,
    )
```

```python
import functools
import heapq

import jax
import jax.numpy as jnp
from jax import lax
from jax.experimental import pallas as pl
from jax.experimental.pallas import tpu as pltpu
from jax.sharding import PartitionSpec as P

HEAD = 256
EPSILON = 1e-06
ADVANCE_RATE = 0.5
LOG_BASE = 9.210340371976184
MESH = pl.DeviceIdType.MESH

RINGS = {"x": 4, "y": 4, "z": 8}
BLOCKS = 128
ROWS = 112
COLS = 512
TOK = 480
WIDTH = 3584
ROUTES = (("xyz", 0, 16), ("yzx", 16, 32), ("yzx", 32, 64), ("xzy", 64, 80), ("xzy", 80, 112))
ROUTE_ORDER = (3, 1, 4, 2, 0)
NR = len(ROUTES)
GROUPS = ((1, 3), (2,), (0, 4))
HAND_TIME = 2.5
HALF_K = WIDTH // 2
STRIPS = ((0, 0, 2), (1, 0, 2), (2, 0, 1), (2, 1, 1), (3, 0, 2), (4, 0, 1), (4, 1, 1))
TABLE_ROWS = ((0, 128), (128, 128), (256, 128), (384, 96))


def reach(ring, sign, parity):
    return ring // 2 if (sign > 0) == (parity % 2 == 0) else ring // 2 - 1


def distance(route, item):
    place = ROUTES[route][0].index("z")
    if item[0] <= place:
        return 0
    return item[place] % 8


def plan():
    rate, latency = 43.5e3, 2.2
    busy, queue, ids = {}, [], {}
    serial = 0

    def push(at, event):
        nonlocal serial
        heapq.heappush(queue, (at, serial, event))
        serial += 1

    def send(at, route, item, axis, sign, outs):
        order, low, high = ROUTES[route]
        size = (high - low) * COLS * 2 * (1 if item[0] == 1 else RINGS[order[0]])
        begin = max(at, busy.get((axis, sign), 0.0))
        busy[axis, sign] = begin + size / rate
        ids[route, item] = len(ids)
        outs.append((item, axis, sign))
        push(busy[axis, sign] + latency, ("item", route, item, sign))

    at = 12.4
    for route in ROUTE_ORDER:
        at += (ROUTES[route][2] - ROUTES[route][1]) / ROWS * 9.8
        push(at, ("own", route, None, 0))
    left, steps, when = {}, [], {}
    missing = {(route, z): 16 for route in range(NR) for z in range(8)}
    fill = [("strip", n, 1.2) for n in range(len(STRIPS))]
    fill += [("table", n, 0.8) for n in range(len(TABLE_ROWS))]
    units = [(group, z) for group in GROUPS for z in range(8)]
    ends = [(0, (0, 1, 7)), (1, (1, 2, 3)), (3, (5, 6, 7)), (2, (3, 4, 5))]
    clock = 9.0
    while queue or units or ends:
        if queue and queue[0][0] <= clock:
            at, _, (kind, route, item, sign) = heapq.heappop(queue)
            clock += 0.12
            one, two, three = ROUTES[route][0]
            outs = []
            if kind == "own":
                clock += 0.2
                left[route] = RINGS[one] - 1
                for s in (1, -1):
                    if reach(RINGS[one], s, route):
                        send(clock, route, (1, s, 0), one, s, outs)
            elif item[0] == 1:
                if abs(item[1]) < reach(RINGS[one], sign, route):
                    send(clock, route, (1, item[1] + sign, 0), one, sign, outs)
                left[route] -= 1
                if left[route] == 0:
                    for s in (1, -1):
                        send(clock, route, (2, s, 0), two, s, outs)
                    for s in (1, -1):
                        send(clock, route, (3, 0, s), three, s, outs)
            elif item[0] == 2:
                if abs(item[1]) < reach(RINGS[two], sign, route + 1):
                    send(clock, route, (2, item[1] + sign, 0), two, sign, outs)
                for s in (1, -1):
                    send(clock, route, (3, item[1], s), three, s, outs)
            else:
                if abs(item[2]) < reach(RINGS[three], sign, item[1]):
                    send(clock, route, (3, item[1], item[2] + sign), three, sign, outs)
            z = distance(route, item or (1, 0, 0))
            missing[route, z] -= 1 if kind == "own" or item[0] == 1 else RINGS[one]
            when[route, z] = clock + HAND_TIME
            steps.append((kind, route, item, outs))
            continue
        soon = queue[0][0] if queue else 1e9
        if fill and (soon - clock >= 0.6 * fill[0][2]):
            steps.append(fill[0][:2])
            clock += fill.pop(0)[2]
            continue
        able = [
            (max(when[route, z] for route in group), group, z)
            for group, z in units
            if not fill and not any(missing[route, z] for route in group)
        ]
        able.sort()
        if able and able[0][0] <= clock:
            _, group, z = able[0]
            tall = sum(ROUTES[route][2] - ROUTES[route][1] for route in group)
            steps.append(("unit", group, z))
            units.remove((group, z))
            clock += 2 * (0.1 + 0.143 * tall / 16)
            for end in [e for e in ends if not any(z in e[1] for _, z in units)]:
                steps.append(("finish", end[0]))
                ends.remove(end)
                clock += 0.5
            continue
        clock = min([soon] + [entry[0] for entry in able])
    return steps, ids


def kernel(
    steps, ids,
    tok_in, fast_in, slow_in, fast_gain_in, slow_gain_in, pos_in,
    q_out, k_out, v_out, weight_out, gain_out,
    *rest,
):
    bufs, rest = rest[:NR], rest[NR:]
    (
        tok, perm, strips, acc, own1, got1, sum2, got2, slow, fast_gain, slow_gain, pos,
        gain, gain_got1, gain_sum, gain_got2, gain_new, turn_c, turn_s, scale,
        load_sem, pair_send, pair_recv, rs_send, rs_recv, item_recv, item_send, hand_send, hand_recv,
    ) = rest
    f = lax.axis_index("fsdp")
    r = lax.axis_index("rep")
    zl, x, y = lax.rem(f, 2), lax.rem(f // 2, 4), f // 8
    zh, c = r // 2, lax.rem(r, 2)
    z = zh * 2 + zl
    at = {"x": x, "y": y, "z": z}

    def device(px, py, pz, pc):
        return ((py * 4 + px) * 2 + lax.rem(pz, 2), (pz // 2) * 2 + pc)

    def wrap(p, off, n):
        return lax.rem(p + (off % n), n)

    def beside(axis, sign):
        p = dict(at)
        p[axis] = wrap(p[axis], sign, RINGS[axis])
        return device(p["x"], p["y"], p["z"], c)

    partner = (f, zh * 2 + 1 - c)
    peers = [(f, wrap(zh, k, 4) * 2 + c) for k in (1, 2, 3)]
    sides = {(a, s): beside(a, s) for a in "xyz" for s in (1, -1)}

    def load(src, dst, sem):
        return pltpu.make_async_copy(src, dst, load_sem.at[sem])

    loads = [
        load(fast_gain_in, fast_gain, 0),
        load(slow_gain_in, slow_gain, 1),
        load(slow_in, slow, 2),
        load(pos_in, pos, 3),
        load(tok_in, tok, 4),
    ]
    mine = []
    for k in range(4):
        cols = pl.ds(pl.multiple_of((k * 2 + c) * COLS, COLS), COLS)
        mine.append(load(fast_in.at[:, cols], own1.at[k], 5 + k))
    barrier = pltpu.get_barrier_semaphore()
    everyone = [partner] + peers + list(sides.values())
    for peer in everyone:
        pl.semaphore_signal(barrier, inc=1, device_id=peer, device_id_type=MESH)
    for copy in loads[:2] + mine + loads[2:]:
        copy.start()

    def clear(b, _):
        acc[b] = jnp.zeros((TOK, COLS), jnp.float32)
        return 0

    lax.fori_loop(0, 8, clear, 0)
    for copy in loads[:2]:
        copy.wait()
    gain[...] = jnp.zeros((8, 128), jnp.float32)
    gain[0:1, 0:14] = slow_gain[...]
    gain[...] = pltpu.roll(gain[...], r * 14, 1)
    gain[1:2, :] = gain[0:1, :]
    gain[0:1, :] = jnp.zeros((1, 128), jnp.float32)
    gain[0:1, 0:ROWS] = fast_gain[...].astype(jnp.float32)
    pl.semaphore_wait(barrier, len(everyone))

    def remote(src, dst, send_sem, recv_sem, peer):
        return pltpu.make_async_remote_copy(
            src_ref=src, dst_ref=dst, send_sem=send_sem, recv_sem=recv_sem,
            device_id=peer, device_id_type=MESH,
        )

    pair = []
    for k in range(4):
        cols = pl.ds(pl.multiple_of((k * 2 + 1 - c) * COLS, COLS), COLS)
        pair.append(remote(fast_in.at[:, cols], got1.at[k], pair_send.at[k], pair_recv.at[k], partner))
    pair.append(remote(gain, gain_got1, pair_send.at[4], pair_recv.at[4], partner))
    for copy in pair:
        copy.start()
    for copy in mine:
        copy.wait()
    for copy in pair:
        copy.wait_recv()
    gain_sum[...] = gain[...] + gain_got1[...]
    for k in (1, 2, 3):
        to = wrap(zh, k, 4)
        sum2[k - 1] = (own1[to].astype(jnp.float32) + got1[to].astype(jnp.float32)).astype(jnp.bfloat16)
    scatter = []
    for n in range(3):
        s = NR * 3 + n
        scatter.append(remote(gain_sum, gain_got2.at[n], rs_send.at[s], rs_recv.at[s], peers[n]))
    for route in ROUTE_ORDER:
        rows = pl.ds(ROUTES[route][1], ROUTES[route][2] - ROUTES[route][1])
        for n in range(3):
            s = route * 3 + n
            scatter.append(
                remote(sum2.at[n, rows], got2.at[n, rows], rs_send.at[s], rs_recv.at[s], peers[n])
            )
    for copy in scatter:
        copy.start()

    def gains():
        loads[2].wait()
        for copy in scatter[:3]:
            copy.wait_recv()
        totals = gain_sum[...] + gain_got2[0] + gain_got2[1] + gain_got2[2]
        old_gain = totals[1:2, :]
        new_gain = old_gain + ADVANCE_RATE * (totals[0:1, :] / 8.0 - old_gain)
        row = 1.0 + new_gain.astype(jnp.bfloat16).astype(jnp.float32)
        eye = lax.broadcasted_iota(jnp.int32, (ROWS, 128), 0) == lax.broadcasted_iota(jnp.int32, (ROWS, 128), 1)
        column = jnp.sum(jnp.where(eye, jnp.broadcast_to(row, (ROWS, 128)), 0.0), axis=1, keepdims=True)
        scale[...] = jnp.broadcast_to(column, (ROWS, 128))
        gain_new[...] = jnp.broadcast_to(new_gain, (8, 128))
        gain_new[...] = pltpu.roll(gain_new[...], lax.rem(128 - r * 14, 128), 1)
        gain_out[...] = gain_new[0:1, 0:14]

    def update(route):
        low, high = ROUTES[route][1:]
        for n in range(3):
            rows = pl.ds(low, high - low)
            remote(
                sum2.at[n, rows], got2.at[n, rows], rs_send.at[route * 3 + n], rs_recv.at[route * 3 + n], peers[n]
            ).wait_recv()
        total = own1[zh, low:high].astype(jnp.float32) + got1[zh, low:high].astype(jnp.float32)
        for n in range(3):
            total = total + got2[n, low:high].astype(jnp.float32)
        old = slow[low:high]
        new = old + ADVANCE_RATE * (total / 8.0 - old)
        weight_out[low:high] = new
        scaled = new.astype(jnp.bfloat16).astype(jnp.float32) * jnp.tile(scale[low:high], (1, COLS // 128))
        bufs[route][c, piece(route, (1, 0, 0))[0]] = scaled.astype(jnp.bfloat16)

    def spot(route, px, py, pz):
        one, two, three = ROUTES[route][0]
        p = {"x": px, "y": py, "z": pz}
        return (p[three] * RINGS[two] + p[two]) * RINGS[one] + p[one]

    def piece(route, item):
        one, two, three = ROUTES[route][0]
        n1, n2, n3 = RINGS[one], RINGS[two], RINGS[three]
        p1, p2, p3 = at[one], at[two], at[three]
        if item[0] == 1:
            return (p3 * n2 + p2) * n1 + wrap(p1, -item[1], n1), 1
        if item[0] == 2:
            return (p3 * n2 + wrap(p2, -item[1], n2)) * n1, n1
        return (wrap(p3, -item[2], n3) * n2 + wrap(p2, -item[1], n2)) * n1, n1

    def view(route, item):
        start, size = piece(route, item)
        return bufs[route].at[c, pl.ds(start, size)]

    def forward(route, item, axis, sign):
        phase, a, b = item
        held = (phase, a - sign, b) if phase < 3 else (phase, a, b - sign)
        part = view(route, held)
        remote(part, part, item_send.at[route], item_recv.at[ids[route, item]], sides[axis, sign]).start()

    def hand(route, item):
        part = view(route, item)
        sem = hand_recv.at[route * 8 + distance(route, item)]
        remote(part, part, hand_send.at[route], sem, partner).start()

    def table(first, count):
        rows = pl.ds(first, count)
        spots = jnp.broadcast_to(pos[0:1, first : first + count].astype(jnp.float32), (count, count))
        eye = lax.broadcasted_iota(jnp.int32, (count, count), 0) == lax.broadcasted_iota(jnp.int32, (count, count), 1)
        place = jnp.sum(jnp.where(eye, spots, 0.0), axis=1, keepdims=True)
        lane = lax.broadcasted_iota(jnp.int32, (1, 128), 1).astype(jnp.float32)
        rates = jnp.exp(lane * (-2.0 / HEAD * LOG_BASE))
        angles = place * rates
        t = tok[rows, :].astype(jnp.float32)
        inv = lax.rsqrt(jnp.sum(t * t, axis=1, keepdims=True) * (1.0 / WIDTH) + EPSILON)
        turn_c[0, rows, :] = jnp.cos(angles) * inv
        turn_s[rows, :] = jnp.sin(angles) * inv
        turn_c[1, rows, :] = jnp.broadcast_to(inv, (count, 128))

    def strip(n):
        route, parity, parities = STRIPS[n]
        low, high = ROUTES[route][1:]
        tall = high - low
        lane = lax.broadcasted_iota(jnp.int32, (1, 256), 1)
        if parities == 2:
            pz, lane = lane // 128, lax.rem(lane, 128)
        else:
            pz = parity
        source = (lane // tall) * (2 * ROWS) + pz * ROWS + low + lax.rem(lane, tall)

        def rows_of(i, _):
            first = pl.multiple_of(i * 128, 128)
            k = lax.broadcasted_iota(jnp.int32, (128, 256), 0) + first
            perm[pl.ds(first, 128), :] = jnp.where(k == source, 1.0, 0.0).astype(jnp.bfloat16)
            return 0

        lax.fori_loop(0, HALF_K // 128, rows_of, 0)
        for p in range(2):
            moved = jnp.dot(
                tok[:, HALF_K * p : HALF_K * (p + 1)], perm[...], preferred_element_type=jnp.float32
            ).astype(jnp.bfloat16)
            to = 16 * low + p * 8 * tall
            if parities == 2:
                strips[0, :, to : to + 128] = moved[:, :128]
                strips[1, :, to : to + 128] = moved[:, 128:]
            else:
                strips[parity, :, to : to + 256] = moved

    def unit(group, far):
        for route in group:
            some = bufs[route].at[1 - c, pl.ds(0, 16)]
            remote(some, some, hand_send.at[route], hand_recv.at[route * 8 + far], partner).wait_recv()
        wz = wrap(z, -far, 8)

        def of_core(bc, _):
            parts = [
                bufs[route][bc, spot(route, px, py, wz)] for route in group for py in range(4) for px in range(4)
            ]
            lanes = [
                strips[lax.rem(wz, 2), :, 16 * ROUTES[route][1] : 16 * ROUTES[route][2]] for route in group
            ]
            acc[(wz // 2) * 2 + bc] += jnp.dot(
                jnp.concatenate(lanes, axis=1), jnp.concatenate(parts, axis=0), preferred_element_type=jnp.float32
            )
            return 0

        lax.fori_loop(0, 2, of_core, 0)

    def finish(far):
        bz = wrap(zh, -far, 4)

        def of_core(bc, _):
            b = bz * 2 + bc

            def turned(ref, first):
                start = (b - first) * COLS
                for h in range(0, COLS, HEAD):
                    u, w = acc[b, :, h : h + 128], acc[b, :, h + 128 : h + 256]
                    tc, ts = turn_c[0], turn_s[...]
                    ref[:, pl.ds(pl.multiple_of(start + h, 128), 128)] = (u * tc - w * ts).astype(jnp.bfloat16)
                    ref[:, pl.ds(pl.multiple_of(start + h + 128, 128), 128)] = (w * tc + u * ts).astype(jnp.bfloat16)

            @pl.when(b < 4)
            def _():
                turned(q_out, 0)

            @pl.when((b >= 4) & (b < 6))
            def _():
                turned(k_out, 4)

            @pl.when(b >= 6)
            def _():
                for h in range(0, COLS, 128):
                    cols = pl.ds(pl.multiple_of((b - 6) * COLS + h, 128), 128)
                    v_out[:, cols] = (acc[b, :, h : h + 128] * turn_c[1]).astype(jnp.bfloat16)

            return 0

        lax.fori_loop(0, 2, of_core, 0)

    first_strip, first_table, first_own = True, True, True
    for step in steps:
        if step[0] == "strip":
            if first_strip:
                loads[4].wait()
                first_strip = False
            strip(step[1])
        elif step[0] == "table":
            if first_table:
                loads[3].wait()
                first_table = False
            table(*TABLE_ROWS[step[1]])
        elif step[0] == "unit":
            unit(*step[1:])
        elif step[0] == "finish":
            finish(step[1])
        else:
            kind, route, item, outs = step
            if kind == "own":
                if first_own:
                    gains()
                    first_own = False
                update(route)
                item = (1, 0, 0)
            else:
                part = view(route, item)
                remote(part, part, item_send.at[route], item_recv.at[ids[route, item]], partner).wait_recv()
            for target, axis, sign in outs:
                forward(route, target, axis, sign)
            hand(route, item)

    for copy in pair + scatter:
        copy.wait_send()
    for route in range(NR):
        most = bufs[route].at[0, pl.ds(0, BLOCKS - 1)]
        remote(most, most, item_send.at[route], item_recv.at[0], partner).wait_send()
        every = bufs[route].at[0]
        remote(every, every, hand_send.at[route], hand_recv.at[0], partner).wait_send()


def flush(*refs):
    sem = refs[-1]
    count = len(refs) // 2
    copies = [pltpu.make_async_copy(refs[n], refs[count + n], sem.at[n]) for n in range(count)]
    for copy in copies:
        copy.start()
    for copy in copies:
        copy.wait()


def on_device(tokens, positions, slow_weight, fast_weight, slow_gain, fast_gain):
    steps, ids = plan()
    f32, bf16 = jnp.float32, jnp.bfloat16
    vmem, dma = pltpu.VMEM, pltpu.SemaphoreType.DMA
    shapes = (
        ((TOK, 2048), bf16),
        ((TOK, 1024), bf16),
        ((TOK, 1024), bf16),
        ((ROWS, COLS), f32),
        ((1, 14), f32),
    )
    held = pl.BlockSpec(memory_space=pltpu.VMEM)
    far = pl.BlockSpec(memory_space=pltpu.HBM)
    results = pl.pallas_call(
        functools.partial(kernel, steps, ids),
        out_shape=tuple(vmem(*s) for s in shapes),
        in_specs=[far] * 6,
        out_specs=(held,) * 5,
        scratch_shapes=[
            *(vmem((2, BLOCKS, high - low, COLS), bf16) for _, low, high in ROUTES),
            vmem((TOK, WIDTH), bf16),
            vmem((HALF_K, 256), bf16),
            vmem((2, TOK, HALF_K), bf16),
            vmem((8, TOK, COLS), f32),
            vmem((4, ROWS, COLS), bf16),
            vmem((4, ROWS, COLS), bf16),
            vmem((3, ROWS, COLS), bf16),
            vmem((3, ROWS, COLS), bf16),
            vmem((ROWS, COLS), f32),
            vmem((1, ROWS), bf16),
            vmem((1, 14), f32),
            vmem((1, TOK), jnp.int32),
            vmem((8, 128), f32),
            vmem((8, 128), f32),
            vmem((8, 128), f32),
            vmem((3, 8, 128), f32),
            vmem((8, 128), f32),
            vmem((2, TOK, 128), f32),
            vmem((TOK, 128), f32),
            vmem((ROWS, 128), f32),
            dma((9,)),
            dma((5,)),
            dma((5,)),
            dma((NR * 3 + 3,)),
            dma((NR * 3 + 3,)),
            dma((len(ids),)),
            dma((NR,)),
            dma((NR,)),
            dma((NR * 8,)),
        ],
        compiler_params=pltpu.CompilerParams(
            collective_id=0, has_side_effects=True, vmem_limit_bytes=57 * 1024 * 1024
        ),
    )(
        tokens, fast_weight[0], slow_weight, fast_gain,
        slow_gain.reshape(1, 14), positions.reshape(1, TOK),
    )
    q, k, v, new_weight, new_gain = pl.pallas_call(
        flush,
        out_shape=tuple(jax.ShapeDtypeStruct(*s) for s in shapes),
        in_specs=[held] * 5,
        out_specs=(far,) * 5,
        scratch_shapes=[dma((5,))],
        compiler_params=pltpu.CompilerParams(vmem_limit_bytes=1024 * 1024),
    )(*results)
    return q, k, v, new_weight, new_gain.reshape(14)


def solution(mesh):
    return jax.shard_map(
        on_device,
        mesh=mesh,
        in_specs=(
            P(("fsdp", "rep"), None),
            P(("fsdp", "rep")),
            P("fsdp", "rep"),
            P("rep", "fsdp", None),
            P(("fsdp", "rep")),
            P("rep", "fsdp"),
        ),
        out_specs=(
            P(("fsdp", "rep"), None),
            P(("fsdp", "rep"), None),
            P(("fsdp", "rep"), None),
            P("fsdp", "rep"),
            P(("fsdp", "rep")),
        ),
        check_vma=False,
    )
```

```python
import functools
import heapq

import jax
import jax.numpy as jnp
from jax import lax
from jax.experimental import pallas as pl
from jax.experimental.pallas import tpu as pltpu
from jax.sharding import PartitionSpec as P

HEAD = 256
EPSILON = 1e-06
ADVANCE_RATE = 0.5
LOG_BASE = 9.210340371976184
MESH = pl.DeviceIdType.MESH

RINGS = {"x": 4, "y": 4, "z": 8}
BLOCKS = 128
ROWS = 112
COLS = 512
TOK = 480
WIDTH = 3584
ROUTES = (("xyz", 0, 16), ("yzx", 16, 32), ("yzx", 32, 64), ("xzy", 64, 80), ("xzy", 80, 112))
ROUTE_ORDER = (3, 1, 4, 2, 0)
NR = len(ROUTES)
GROUPS = ((1, 3), (0, 2, 4))
HAND_TIME = 2.0
HALF_K = WIDTH // 2
STRIPS = ((0, 0, 2), (1, 0, 2), (2, 0, 1), (2, 1, 1), (3, 0, 2), (4, 0, 1), (4, 1, 1))
TABLE_ROWS = ((0, 128), (128, 128), (256, 128), (384, 96))


def reach(ring, sign, parity):
    return ring // 2 if (sign > 0) == (parity % 2 == 0) else ring // 2 - 1


def distance(route, item):
    place = ROUTES[route][0].index("z")
    if item[0] <= place:
        return 0
    return item[place] % 8


def plan():
    rate, latency = 43.5e3, 2.2
    busy, queue, ids = {}, [], {}
    serial = 0

    def push(at, event):
        nonlocal serial
        heapq.heappush(queue, (at, serial, event))
        serial += 1

    def send(at, route, item, axis, sign, outs):
        order, low, high = ROUTES[route]
        size = (high - low) * COLS * 2 * (1 if item[0] == 1 else RINGS[order[0]])
        begin = max(at, busy.get((axis, sign), 0.0))
        busy[axis, sign] = begin + size / rate
        ids[route, item] = len(ids)
        outs.append((item, axis, sign))
        push(busy[axis, sign] + latency, ("item", route, item, sign))

    at = 12.4
    for route in ROUTE_ORDER:
        at += (ROUTES[route][2] - ROUTES[route][1]) / ROWS * 9.8
        push(at, ("own", route, None, 0))
    left, steps, when = {}, [], {}
    missing = {(route, z): 16 for route in range(NR) for z in range(8)}
    fill = [("strip", n, 1.2) for n in range(len(STRIPS))]
    fill += [("table", n, 0.8) for n in range(len(TABLE_ROWS))]
    units = [(group, z, side) for group in GROUPS for z in range(8) for side in (0, 1)]
    need = ((0, (0, 1, 7)), (1, (1, 2, 3)), (3, (5, 6, 7)), (2, (3, 4, 5)))
    ends = [(far, zs, side) for far, zs in need for side in (0, 1)]
    clock = 9.0
    while queue or units or ends:
        if queue and queue[0][0] <= clock:
            at, _, (kind, route, item, sign) = heapq.heappop(queue)
            clock += 0.12
            one, two, three = ROUTES[route][0]
            outs = []
            if kind == "own":
                clock += 0.2
                left[route] = RINGS[one] - 1
                for s in (1, -1):
                    if reach(RINGS[one], s, route):
                        send(clock, route, (1, s, 0), one, s, outs)
            elif item[0] == 1:
                if abs(item[1]) < reach(RINGS[one], sign, route):
                    send(clock, route, (1, item[1] + sign, 0), one, sign, outs)
                left[route] -= 1
                if left[route] == 0:
                    for s in (1, -1):
                        send(clock, route, (2, s, 0), two, s, outs)
                    for s in (1, -1):
                        send(clock, route, (3, 0, s), three, s, outs)
            elif item[0] == 2:
                if abs(item[1]) < reach(RINGS[two], sign, route + 1):
                    send(clock, route, (2, item[1] + sign, 0), two, sign, outs)
                for s in (1, -1):
                    send(clock, route, (3, item[1], s), three, s, outs)
            else:
                if abs(item[2]) < reach(RINGS[three], sign, item[1]):
                    send(clock, route, (3, item[1], item[2] + sign), three, sign, outs)
            z = distance(route, item or (1, 0, 0))
            missing[route, z] -= 1 if kind == "own" or item[0] == 1 else RINGS[one]
            when[route, z] = clock
            steps.append((kind, route, item, outs))
            continue
        soon = queue[0][0] if queue else 1e9
        if fill and (soon - clock >= 0.6 * fill[0][2]):
            steps.append(fill[0][:2])
            clock += fill.pop(0)[2]
            continue
        able = [
            (max(when[route, z] for route in group) + HAND_TIME * side, group, z, side)
            for group, z, side in units
            if not fill and not any(missing[route, z] for route in group)
        ]
        able.sort()
        if able and able[0][0] <= clock:
            _, group, z, side = able[0]
            tall = sum(ROUTES[route][2] - ROUTES[route][1] for route in group)
            steps.append(("unit", group, z, side))
            units.remove((group, z, side))
            clock += 0.1 + 0.143 * tall / 16
            for end in [e for e in ends if not any(u[1] in e[1] and u[2] == e[2] for u in units)]:
                steps.append(("finish", end[0], end[2]))
                ends.remove(end)
                clock += 0.25
            continue
        clock = min([soon] + [entry[0] for entry in able])
    return steps, ids


def kernel(
    steps, ids,
    tok_in, fast_in, slow_in, fast_gain_in, slow_gain_in, pos_in,
    q_out, k_out, v_out, weight_out, gain_out,
    *rest,
):
    bufs, rest = rest[:NR], rest[NR:]
    (
        tok, perm, strips, acc, own1, got1, sum2, got2, slow, fast_gain, slow_gain, pos,
        gain, gain_got1, gain_sum, gain_got2, gain_new, turn_c, turn_s, scale,
        load_sem, pair_send, pair_recv, rs_send, rs_recv, item_recv, item_send, hand_send, hand_recv,
    ) = rest
    f = lax.axis_index("fsdp")
    r = lax.axis_index("rep")
    zl, x, y = lax.rem(f, 2), lax.rem(f // 2, 4), f // 8
    zh, c = r // 2, lax.rem(r, 2)
    z = zh * 2 + zl
    at = {"x": x, "y": y, "z": z}

    def device(px, py, pz, pc):
        return ((py * 4 + px) * 2 + lax.rem(pz, 2), (pz // 2) * 2 + pc)

    def wrap(p, off, n):
        return lax.rem(p + (off % n), n)

    def beside(axis, sign):
        p = dict(at)
        p[axis] = wrap(p[axis], sign, RINGS[axis])
        return device(p["x"], p["y"], p["z"], c)

    partner = (f, zh * 2 + 1 - c)
    peers = [(f, wrap(zh, k, 4) * 2 + c) for k in (1, 2, 3)]
    sides = {(a, s): beside(a, s) for a in "xyz" for s in (1, -1)}

    def load(src, dst, sem):
        return pltpu.make_async_copy(src, dst, load_sem.at[sem])

    loads = [
        load(fast_gain_in, fast_gain, 0),
        load(slow_gain_in, slow_gain, 1),
        load(slow_in, slow, 2),
        load(pos_in, pos, 3),
        load(tok_in, tok, 4),
    ]
    mine = []
    for k in range(4):
        cols = pl.ds(pl.multiple_of((k * 2 + c) * COLS, COLS), COLS)
        mine.append(load(fast_in.at[:, cols], own1.at[k], 5 + k))
    barrier = pltpu.get_barrier_semaphore()
    everyone = [partner] + peers + list(sides.values())
    for peer in everyone:
        pl.semaphore_signal(barrier, inc=1, device_id=peer, device_id_type=MESH)
    for copy in loads[:2] + mine + loads[2:]:
        copy.start()

    def clear(b, _):
        acc[b] = jnp.zeros((TOK, COLS), jnp.float32)
        return 0

    lax.fori_loop(0, 8, clear, 0)
    for copy in loads[:2]:
        copy.wait()
    gain[...] = jnp.zeros((8, 128), jnp.float32)
    gain[0:1, 0:14] = slow_gain[...]
    gain[...] = pltpu.roll(gain[...], r * 14, 1)
    gain[1:2, :] = gain[0:1, :]
    gain[0:1, :] = jnp.zeros((1, 128), jnp.float32)
    gain[0:1, 0:ROWS] = fast_gain[...].astype(jnp.float32)
    pl.semaphore_wait(barrier, len(everyone))

    def remote(src, dst, send_sem, recv_sem, peer):
        return pltpu.make_async_remote_copy(
            src_ref=src, dst_ref=dst, send_sem=send_sem, recv_sem=recv_sem,
            device_id=peer, device_id_type=MESH,
        )

    pair = []
    for k in range(4):
        cols = pl.ds(pl.multiple_of((k * 2 + 1 - c) * COLS, COLS), COLS)
        pair.append(remote(fast_in.at[:, cols], got1.at[k], pair_send.at[k], pair_recv.at[k], partner))
    pair.append(remote(gain, gain_got1, pair_send.at[4], pair_recv.at[4], partner))
    for copy in pair:
        copy.start()
    for copy in mine:
        copy.wait()
    for copy in pair:
        copy.wait_recv()
    gain_sum[...] = gain[...] + gain_got1[...]
    for k in (1, 2, 3):
        to = wrap(zh, k, 4)
        sum2[k - 1] = (own1[to].astype(jnp.float32) + got1[to].astype(jnp.float32)).astype(jnp.bfloat16)
    scatter = []
    for n in range(3):
        s = NR * 3 + n
        scatter.append(remote(gain_sum, gain_got2.at[n], rs_send.at[s], rs_recv.at[s], peers[n]))
    for route in ROUTE_ORDER:
        rows = pl.ds(ROUTES[route][1], ROUTES[route][2] - ROUTES[route][1])
        for n in range(3):
            s = route * 3 + n
            scatter.append(
                remote(sum2.at[n, rows], got2.at[n, rows], rs_send.at[s], rs_recv.at[s], peers[n])
            )
    for copy in scatter:
        copy.start()

    def gains():
        loads[2].wait()
        for copy in scatter[:3]:
            copy.wait_recv()
        totals = gain_sum[...] + gain_got2[0] + gain_got2[1] + gain_got2[2]
        old_gain = totals[1:2, :]
        new_gain = old_gain + ADVANCE_RATE * (totals[0:1, :] / 8.0 - old_gain)
        row = 1.0 + new_gain.astype(jnp.bfloat16).astype(jnp.float32)
        eye = lax.broadcasted_iota(jnp.int32, (ROWS, 128), 0) == lax.broadcasted_iota(jnp.int32, (ROWS, 128), 1)
        column = jnp.sum(jnp.where(eye, jnp.broadcast_to(row, (ROWS, 128)), 0.0), axis=1, keepdims=True)
        scale[...] = jnp.broadcast_to(column, (ROWS, 128))
        gain_new[...] = jnp.broadcast_to(new_gain, (8, 128))
        gain_new[...] = pltpu.roll(gain_new[...], lax.rem(128 - r * 14, 128), 1)
        gain_out[...] = gain_new[0:1, 0:14]

    def update(route):
        low, high = ROUTES[route][1:]
        for n in range(3):
            rows = pl.ds(low, high - low)
            remote(
                sum2.at[n, rows], got2.at[n, rows], rs_send.at[route * 3 + n], rs_recv.at[route * 3 + n], peers[n]
            ).wait_recv()
        total = own1[zh, low:high].astype(jnp.float32) + got1[zh, low:high].astype(jnp.float32)
        for n in range(3):
            total = total + got2[n, low:high].astype(jnp.float32)
        old = slow[low:high]
        new = old + ADVANCE_RATE * (total / 8.0 - old)
        weight_out[low:high] = new
        scaled = new.astype(jnp.bfloat16).astype(jnp.float32) * jnp.tile(scale[low:high], (1, COLS // 128))
        bufs[route][c, piece(route, (1, 0, 0))[0]] = scaled.astype(jnp.bfloat16)

    def spot(route, px, py, pz):
        one, two, three = ROUTES[route][0]
        p = {"x": px, "y": py, "z": pz}
        return (p[three] * RINGS[two] + p[two]) * RINGS[one] + p[one]

    def piece(route, item):
        one, two, three = ROUTES[route][0]
        n1, n2, n3 = RINGS[one], RINGS[two], RINGS[three]
        p1, p2, p3 = at[one], at[two], at[three]
        if item[0] == 1:
            return (p3 * n2 + p2) * n1 + wrap(p1, -item[1], n1), 1
        if item[0] == 2:
            return (p3 * n2 + wrap(p2, -item[1], n2)) * n1, n1
        return (wrap(p3, -item[2], n3) * n2 + wrap(p2, -item[1], n2)) * n1, n1

    def view(route, item):
        start, size = piece(route, item)
        return bufs[route].at[c, pl.ds(start, size)]

    def forward(route, item, axis, sign):
        phase, a, b = item
        held = (phase, a - sign, b) if phase < 3 else (phase, a, b - sign)
        part = view(route, held)
        remote(part, part, item_send.at[route], item_recv.at[ids[route, item]], sides[axis, sign]).start()

    def hand(route, item):
        part = view(route, item)
        sem = hand_recv.at[route * 8 + distance(route, item)]
        remote(part, part, hand_send.at[route], sem, partner).start()

    def table(first, count):
        rows = pl.ds(first, count)
        spots = jnp.broadcast_to(pos[0:1, first : first + count].astype(jnp.float32), (count, count))
        eye = lax.broadcasted_iota(jnp.int32, (count, count), 0) == lax.broadcasted_iota(jnp.int32, (count, count), 1)
        place = jnp.sum(jnp.where(eye, spots, 0.0), axis=1, keepdims=True)
        lane = lax.broadcasted_iota(jnp.int32, (1, 128), 1).astype(jnp.float32)
        rates = jnp.exp(lane * (-2.0 / HEAD * LOG_BASE))
        angles = place * rates
        t = tok[rows, :].astype(jnp.float32)
        inv = lax.rsqrt(jnp.sum(t * t, axis=1, keepdims=True) * (1.0 / WIDTH) + EPSILON)
        turn_c[0, rows, :] = jnp.cos(angles) * inv
        turn_s[rows, :] = jnp.sin(angles) * inv
        turn_c[1, rows, :] = jnp.broadcast_to(inv, (count, 128))

    def strip(n):
        route, parity, parities = STRIPS[n]
        low, high = ROUTES[route][1:]
        tall = high - low
        lane = lax.broadcasted_iota(jnp.int32, (1, 256), 1)
        if parities == 2:
            pz, lane = lane // 128, lax.rem(lane, 128)
        else:
            pz = parity
        source = (lane // tall) * (2 * ROWS) + pz * ROWS + low + lax.rem(lane, tall)

        def rows_of(i, _):
            first = pl.multiple_of(i * 128, 128)
            k = lax.broadcasted_iota(jnp.int32, (128, 256), 0) + first
            perm[pl.ds(first, 128), :] = jnp.where(k == source, 1.0, 0.0).astype(jnp.bfloat16)
            return 0

        lax.fori_loop(0, HALF_K // 128, rows_of, 0)
        for p in range(2):
            moved = jnp.dot(
                tok[:, HALF_K * p : HALF_K * (p + 1)], perm[...], preferred_element_type=jnp.float32
            ).astype(jnp.bfloat16)
            to = 16 * low + p * 8 * tall
            if parities == 2:
                strips[0, :, to : to + 128] = moved[:, :128]
                strips[1, :, to : to + 128] = moved[:, 128:]
            else:
                strips[parity, :, to : to + 256] = moved

    def unit(group, far, side):
        if side:
            for route in group:
                some = bufs[route].at[1 - c, pl.ds(0, 16)]
                remote(some, some, hand_send.at[route], hand_recv.at[route * 8 + far], partner).wait_recv()
        wz = wrap(z, -far, 8)
        bc = 1 - c if side else c
        parts = [bufs[route][bc, spot(route, px, py, wz)] for route in group for py in range(4) for px in range(4)]
        lanes = [strips[lax.rem(wz, 2), :, 16 * ROUTES[route][1] : 16 * ROUTES[route][2]] for route in group]
        acc[(wz // 2) * 2 + bc] += jnp.dot(
            jnp.concatenate(lanes, axis=1), jnp.concatenate(parts, axis=0), preferred_element_type=jnp.float32
        )

    def finish(far, side):
        b = wrap(zh, -far, 4) * 2 + (1 - c if side else c)

        def turned(ref, first):
            start = (b - first) * COLS
            for h in range(0, COLS, HEAD):
                u, w = acc[b, :, h : h + 128], acc[b, :, h + 128 : h + 256]
                tc, ts = turn_c[0], turn_s[...]
                ref[:, pl.ds(pl.multiple_of(start + h, 128), 128)] = (u * tc - w * ts).astype(jnp.bfloat16)
                ref[:, pl.ds(pl.multiple_of(start + h + 128, 128), 128)] = (w * tc + u * ts).astype(jnp.bfloat16)

        @pl.when(b < 4)
        def _():
            turned(q_out, 0)

        @pl.when((b >= 4) & (b < 6))
        def _():
            turned(k_out, 4)

        @pl.when(b >= 6)
        def _():
            for h in range(0, COLS, 128):
                cols = pl.ds(pl.multiple_of((b - 6) * COLS + h, 128), 128)
                v_out[:, cols] = (acc[b, :, h : h + 128] * turn_c[1]).astype(jnp.bfloat16)

    first_strip, first_table, first_own = True, True, True
    for step in steps:
        if step[0] == "strip":
            if first_strip:
                loads[4].wait()
                first_strip = False
            strip(step[1])
        elif step[0] == "table":
            if first_table:
                loads[3].wait()
                first_table = False
            table(*TABLE_ROWS[step[1]])
        elif step[0] == "unit":
            unit(*step[1:])
        elif step[0] == "finish":
            finish(*step[1:])
        else:
            kind, route, item, outs = step
            if kind == "own":
                if first_own:
                    gains()
                    first_own = False
                update(route)
                item = (1, 0, 0)
            else:
                part = view(route, item)
                remote(part, part, item_send.at[route], item_recv.at[ids[route, item]], partner).wait_recv()
            for target, axis, sign in outs:
                forward(route, target, axis, sign)
            hand(route, item)

    for copy in pair + scatter:
        copy.wait_send()
    for route in range(NR):
        most = bufs[route].at[0, pl.ds(0, BLOCKS - 1)]
        remote(most, most, item_send.at[route], item_recv.at[0], partner).wait_send()
        every = bufs[route].at[0]
        remote(every, every, hand_send.at[route], hand_recv.at[0], partner).wait_send()


def flush(*refs):
    sem = refs[-1]
    count = len(refs) // 2
    copies = [pltpu.make_async_copy(refs[n], refs[count + n], sem.at[n]) for n in range(count)]
    for copy in copies:
        copy.start()
    for copy in copies:
        copy.wait()


def on_device(tokens, positions, slow_weight, fast_weight, slow_gain, fast_gain):
    steps, ids = plan()
    f32, bf16 = jnp.float32, jnp.bfloat16
    vmem, dma = pltpu.VMEM, pltpu.SemaphoreType.DMA
    shapes = (
        ((TOK, 2048), bf16),
        ((TOK, 1024), bf16),
        ((TOK, 1024), bf16),
        ((ROWS, COLS), f32),
        ((1, 14), f32),
    )
    held = pl.BlockSpec(memory_space=pltpu.VMEM)
    far = pl.BlockSpec(memory_space=pltpu.HBM)
    results = pl.pallas_call(
        functools.partial(kernel, steps, ids),
        out_shape=tuple(vmem(*s) for s in shapes),
        in_specs=[far] * 6,
        out_specs=(held,) * 5,
        scratch_shapes=[
            *(vmem((2, BLOCKS, high - low, COLS), bf16) for _, low, high in ROUTES),
            vmem((TOK, WIDTH), bf16),
            vmem((HALF_K, 256), bf16),
            vmem((2, TOK, HALF_K), bf16),
            vmem((8, TOK, COLS), f32),
            vmem((4, ROWS, COLS), bf16),
            vmem((4, ROWS, COLS), bf16),
            vmem((3, ROWS, COLS), bf16),
            vmem((3, ROWS, COLS), bf16),
            vmem((ROWS, COLS), f32),
            vmem((1, ROWS), bf16),
            vmem((1, 14), f32),
            vmem((1, TOK), jnp.int32),
            vmem((8, 128), f32),
            vmem((8, 128), f32),
            vmem((8, 128), f32),
            vmem((3, 8, 128), f32),
            vmem((8, 128), f32),
            vmem((2, TOK, 128), f32),
            vmem((TOK, 128), f32),
            vmem((ROWS, 128), f32),
            dma((9,)),
            dma((5,)),
            dma((5,)),
            dma((NR * 3 + 3,)),
            dma((NR * 3 + 3,)),
            dma((len(ids),)),
            dma((NR,)),
            dma((NR,)),
            dma((NR * 8,)),
        ],
        compiler_params=pltpu.CompilerParams(
            collective_id=0, has_side_effects=True, vmem_limit_bytes=57 * 1024 * 1024
        ),
    )(
        tokens, fast_weight[0], slow_weight, fast_gain,
        slow_gain.reshape(1, 14), positions.reshape(1, TOK),
    )
    q, k, v, new_weight, new_gain = pl.pallas_call(
        flush,
        out_shape=tuple(jax.ShapeDtypeStruct(*s) for s in shapes),
        in_specs=[held] * 5,
        out_specs=(far,) * 5,
        scratch_shapes=[dma((5,))],
        compiler_params=pltpu.CompilerParams(vmem_limit_bytes=1024 * 1024),
    )(*results)
    return q, k, v, new_weight, new_gain.reshape(14)


def solution(mesh):
    return jax.shard_map(
        on_device,
        mesh=mesh,
        in_specs=(
            P(("fsdp", "rep"), None),
            P(("fsdp", "rep")),
            P("fsdp", "rep"),
            P("rep", "fsdp", None),
            P(("fsdp", "rep")),
            P("rep", "fsdp"),
        ),
        out_specs=(
            P(("fsdp", "rep"), None),
            P(("fsdp", "rep"), None),
            P(("fsdp", "rep"), None),
            P("fsdp", "rep"),
            P(("fsdp", "rep")),
        ),
        check_vma=False,
    )
```
